32 devices in a mesh: leaf: 16 (over z, y, x), blk: 2 (over core).
Axes of the slice: x: 2, y: 2, z: 4, core: 2. Of those that a mesh axis runs over, the one named last changes fastest.
Arguments:
- sketch: bfloat16 [16384, 512], P(('leaf', 'blk')), may hold values from -6 to 6
- near_block: bfloat16 [16384, 1024], P(('leaf', 'blk')), may hold values from -0.125 to 0.125
- next_block: bfloat16 [16384, 1024], P(('leaf', 'blk')), may hold values from -0.125 to 0.125
- link_own: bfloat16 [4096, 1024], P('leaf', 'blk')
- link_next: bfloat16 [4096, 1024], P('leaf', 'blk')
- diag_block: float32 [4096, 128], P(('leaf', 'blk'))
- sub_block: float32 [4096, 128], P(('leaf', 'blk'))
- leaf_skeleton: int32 [16, 128], P('leaf'), may hold values from 0 to 1023, as said below
- merge_skeleton: int32 [16, 4, 128], P('leaf'), may hold values from 0 to 255, as said below
Outputs:
- samples: float32 [16384, 512], P(('leaf', 'blk'))
- leaf_interp: float32 [16384, 128], P(('leaf', 'blk'))
- merge_interp: float32 [32, 4, 256, 128], P(('leaf', 'blk'))
The draws below stay inside these ranges and needn't reach their ends.
Inputs may be any that keep to these rules, and one draw needn't show every extreme that they name: `leaf_skeleton`: each row holds 128 distinct numbers. `merge_skeleton`: for each row p and level index j, the 128 numbers are distinct; rows p and q with p // 2^(j+1) == q // 2^(j+1) hold equal entries at level index j.
All inputs are finite; a program needn't handle non-finite values.
Results may differ from the reference program's by a relative error of at most 0.0027.
Values may be sent and summed in bfloat16 or wider, within the bound.
A program may use at most 64 MiB of HBM per device.

```python
import math
import jax
import jax.numpy as jnp
from jax import lax

LEAF_ROWS = 1024
SAMPLES = 512
SKEL_RANK = 128
LEVELS = 4
INT_DEV = 128
IFACE_ROWS = 1024
INTERFACE = 16384
INT_ROWS = 256
INTERIOR = 4096
LEAF_PAIRS = 16
N_LEAF = 16
N_BLK = 2


def link_values(key):
    spread = 2.1 * (2.0 * IFACE_ROWS * INT_ROWS) ** (-0.25)
    values = jax.random.normal(key, (INTERIOR, IFACE_ROWS), jnp.float32) * spread
    return values.astype(jnp.bfloat16)


def draw_link_own(key, part):
    return link_values(jax.random.fold_in(key, 1))


def draw_link_next(key, part):
    return link_values(jax.random.fold_in(key, 2))


def draw_diag_block(key, part):
    first_key, second_key = jax.random.split(jax.random.fold_in(key, 11))
    blocks = INTERIOR // INT_DEV
    below = jax.random.normal(first_key, (blocks, INT_DEV, INT_DEV), jnp.float32) / math.sqrt(INT_DEV)
    middle = jax.random.uniform(second_key, (blocks, INT_DEV), jnp.float32, 2.0, 4.0)
    row_index = lax.broadcasted_iota(jnp.int32, (INT_DEV, INT_DEV), 0)
    col_index = lax.broadcasted_iota(jnp.int32, (INT_DEV, INT_DEV), 1)
    lower_part = jnp.where(row_index > col_index, below, 0.0) + jnp.where(row_index == col_index, middle[:, :, None], 0.0)
    return lower_part.reshape(INTERIOR, INT_DEV)


def draw_sub_block(key, part):
    values = jax.random.normal(jax.random.fold_in(key, 12), (INTERIOR, INT_DEV), jnp.float32)
    return values * (1.5 / math.sqrt(INT_DEV))


def distinct_first(key, row_total, choose_from, how_many):
    scores = jax.random.randint(key, (row_total, choose_from), 0, 1 << 20) * choose_from
    scores = scores + lax.broadcasted_iota(jnp.int32, (row_total, choose_from), 1)
    order = jnp.argsort(scores, axis=1)
    return order[:, :how_many].astype(jnp.int32)


def draw_leaf_skeleton(key, part):
    return distinct_first(jax.random.fold_in(key, 21), LEAF_PAIRS, LEAF_ROWS, SKEL_RANK)


def draw_merge_skeleton(key, part):
    tables = []
    for level_index in range(LEVELS):
        span = 2 ** (level_index + 1)
        table = distinct_first(jax.random.fold_in(key, 31 + level_index), LEAF_PAIRS // span, 2 * SKEL_RANK, SKEL_RANK)
        tables.append(jnp.repeat(table, span, axis=0))
    return jnp.stack(tables, axis=1)


def block_scale(rng, dims, cuts, low, high):
    gain = 1.0
    for axis_at, shards_of in cuts:
        draws = jax.random.uniform(jax.random.fold_in(jax.random.fold_in(rng, 6), axis_at), (shards_of,), jnp.float32, low / len(cuts), high / len(cuts))
        gain = gain * jnp.repeat(jnp.exp(draws), dims[axis_at] // shards_of).reshape((-1,) + (1,) * (len(dims) - 1 - axis_at))
    return gain


def gaussian(own_key, dims, width, limit, shards=(), held_as=jnp.bfloat16):
    factor_of = block_scale(own_key, dims, shards, -0.22, 0.18) if shards else 1.0
    result = jax.random.normal(own_key, dims, jnp.float32) * width * factor_of
    return jnp.minimum(jnp.maximum(result, -limit), limit).astype(held_as)


def setup_inputs(seed: int = 0) -> dict:
    key_list = jax.random.split(jax.random.key(seed), 10)
    return {
        "sketch": gaussian(key_list[0], (INTERFACE, SAMPLES), 1.0, 6.0, ((0, 32),)),
        "near_block": gaussian(key_list[1], (INTERFACE, IFACE_ROWS), (2 * IFACE_ROWS) ** -0.5, 0.125, ((0, 32),)),
        "next_block": gaussian(key_list[2], (INTERFACE, IFACE_ROWS), (2 * IFACE_ROWS) ** -0.5, 0.125, ((0, 32),)),
        "link_own": draw_link_own(jax.random.fold_in(key_list[9], 71), 0),
        "link_next": draw_link_next(jax.random.fold_in(key_list[9], 71), 0),
        "diag_block": draw_diag_block(jax.random.fold_in(key_list[9], 71), 0),
        "sub_block": draw_sub_block(jax.random.fold_in(key_list[9], 71), 0),
        "leaf_skeleton": draw_leaf_skeleton(jax.random.fold_in(key_list[9], 71), 0),
        "merge_skeleton": draw_merge_skeleton(jax.random.fold_in(key_list[9], 71), 0),
    }


highest = lax.Precision.HIGHEST

def interp_rows(candidates, chosen):
    gram_matrix = jnp.dot(chosen, chosen.T, precision=highest)
    factor = jnp.linalg.cholesky(gram_matrix)
    cross_term = jnp.dot(chosen, candidates.T, precision=highest)
    return jax.scipy.linalg.cho_solve((factor, True), cross_term).T

def group_terms(operands):
    own_sketch, next_sketch, near_rows, next_rows, link_first, link_second, diag_rows, sub_rows = operands
    direct = jnp.dot(near_rows.astype(jnp.float32), own_sketch.astype(jnp.float32), preferred_element_type=jnp.float32) + jnp.dot(next_rows.astype(jnp.float32), next_sketch.astype(jnp.float32), preferred_element_type=jnp.float32)
    load_sum = jnp.dot(link_first.astype(jnp.float32), own_sketch.astype(jnp.float32), preferred_element_type=jnp.float32) + jnp.dot(link_second.astype(jnp.float32), next_sketch.astype(jnp.float32), preferred_element_type=jnp.float32)
    load_blocks = load_sum.reshape(N_BLK, INT_DEV, SAMPLES)
    diag_blocks = diag_rows.reshape(N_BLK, INT_DEV, INT_DEV)
    sub_blocks = sub_rows.reshape(N_BLK, INT_DEV, INT_DEV)
    forward_list = []
    previous = None
    for block_index in range(N_BLK):
        if block_index == 0:
            right_side = load_blocks[0]
        else:
            right_side = load_blocks[block_index] - jnp.dot(sub_blocks[block_index], previous, precision=highest)
        previous = jax.scipy.linalg.solve_triangular(diag_blocks[block_index], right_side, lower=True)
        forward_list.append(previous)
    backward_list = [None] * N_BLK
    following = None
    for block_index in range(N_BLK - 1, -1, -1):
        if block_index == N_BLK - 1:
            right_side = forward_list[block_index]
        else:
            right_side = forward_list[block_index] - jnp.dot(sub_blocks[block_index + 1].T, following, precision=highest)
        following = jax.scipy.linalg.solve_triangular(diag_blocks[block_index], right_side, lower=True, trans='T')
        backward_list[block_index] = following
    weights = jnp.concatenate(backward_list, axis=0).astype(jnp.bfloat16)
    own_back = jnp.dot(link_first.T.astype(jnp.float32), weights.astype(jnp.float32), preferred_element_type=jnp.float32)
    next_back = jnp.dot(link_second.T.astype(jnp.float32), weights.astype(jnp.float32), preferred_element_type=jnp.float32)
    return (direct, own_back, next_back)

def reference(sketch, near_block, next_block, link_own, link_next, diag_block, sub_block, leaf_skeleton, merge_skeleton):
    group_sketch = sketch.reshape(N_LEAF, IFACE_ROWS, SAMPLES)
    following_sketch = jnp.roll(group_sketch, -1, axis=0)
    direct, own_back, next_back = lax.map(group_terms, (group_sketch, following_sketch, near_block.reshape(N_LEAF, IFACE_ROWS, IFACE_ROWS), next_block.reshape(N_LEAF, IFACE_ROWS, IFACE_ROWS), link_own.reshape(N_LEAF, INT_ROWS, IFACE_ROWS), link_next.reshape(N_LEAF, INT_ROWS, IFACE_ROWS), diag_block.reshape(N_LEAF, INT_ROWS, INT_DEV), sub_block.reshape(N_LEAF, INT_ROWS, INT_DEV)))
    samples = (direct - own_back - jnp.roll(next_back, 1, axis=0)).reshape(INTERFACE, SAMPLES)
    leaf_rows = samples.reshape(LEAF_PAIRS, LEAF_ROWS, SAMPLES)
    chosen = jnp.take_along_axis(leaf_rows, leaf_skeleton.astype(jnp.int32)[:, :, None], axis=1)
    leaf_interp = lax.map(lambda pair: interp_rows(pair[0], pair[1]), (leaf_rows, chosen)).reshape(INTERFACE, SKEL_RANK)
    level_list = []
    for level_index in range(LEVELS):
        candidates = chosen.reshape(-1, 2 * SKEL_RANK, SAMPLES)
        picks = merge_skeleton[::2 ** (level_index + 1), level_index, :].astype(jnp.int32)
        chosen = jnp.take_along_axis(candidates, picks[:, :, None], axis=1)
        matrices = jax.vmap(interp_rows)(candidates, chosen)
        level_list.append(jnp.repeat(matrices, 2 ** (level_index + 2), axis=0))
    merge_interp = jnp.stack(level_list, axis=1)
    return (samples, leaf_interp, merge_interp)
```

```python
import functools

import jax
import jax.numpy as jnp
from jax import lax
from jax.experimental import pallas as pl
from jax.experimental.pallas import tpu as pltpu
from jax.sharding import PartitionSpec as P

highest = lax.Precision.HIGHEST
f32 = jnp.float32
contract_rows = (((0,), (0,)), ((), ()))
contract_cols = (((1,), (1,)), ((), ()))
VMEM_SPEC = pl.BlockSpec(memory_space=pltpu.VMEM)
SMEM_SPEC = pl.BlockSpec(memory_space=pltpu.SMEM)


def shifted(block, axis, distance):
    count = lax.axis_size(axis)
    return lax.ppermute(block, axis, [((i - distance) % count, i) for i in range(count)])


def from_partner(block, axis, apart):
    count = lax.axis_size(axis)
    return lax.ppermute(block, axis, [(i, i ^ 1 << apart) for i in range(count)])


def gathered(block):
    if lax.axis_size("blk") != 2:
        return lax.all_gather(block, "blk", axis=0, tiled=True)
    other = from_partner(block, "blk", 0)
    first = lax.axis_index("blk") == 0
    return jnp.concatenate(
        [jnp.where(first, block, other), jnp.where(first, other, block)], axis=0
    )


def invert_in_place(refs):
    size = refs[0].shape[-1]
    lane = lax.broadcasted_iota(jnp.int32, (1, size), 1)
    for k in range(0, size, 2):
        at0, at1 = lane == k, lane == k + 1
        pivot_cols = at0 | at1
        for ref in refs:
            value = ref[...]
            r0, r1 = value[k : k + 1, :], value[k + 1 : k + 2, :]
            p00, p01 = r0[:, k : k + 1], r0[:, k + 1 : k + 2]
            p10, p11 = r1[:, k : k + 1], r1[:, k + 1 : k + 2]
            q0 = 1.0 / p00
            ratio = p10 * q0
            q1 = 1.0 / (p11 - ratio * p01)
            r0 = jnp.where(pivot_cols, jnp.where(at0, 1.0, 0.0), r0)
            r1 = jnp.where(pivot_cols, jnp.where(at1, 1.0, 0.0), r1)
            new1 = (r1 - ratio * r0) * q1
            new0 = (r0 - p01 * new1) * q0
            ref[...] = (
                jnp.where(pivot_cols, 0.0, value)
                - value[:, k : k + 1] * new0
                - value[:, k + 1 : k + 2] * new1
            )
            ref[k : k + 1, :] = new0
            ref[k + 1 : k + 2, :] = new1


def factor_kernel(diag_ref, sub_ref, out_ref, *work):
    size = diag_ref.shape[1]
    blocks = diag_ref.shape[0] // size
    row = lax.broadcasted_iota(jnp.int32, (size, size), 0)
    col = lax.broadcasted_iota(jnp.int32, (size, size), 1)
    for k in range(blocks):
        work[k][...] = jnp.where(row >= col, diag_ref[k * size : (k + 1) * size, :], 0.0)
    invert_in_place(work)
    out_ref[...] = jnp.zeros_like(out_ref)
    for k in range(blocks):
        rows = slice(k * size, (k + 1) * size)
        inverse = work[k][...]
        out_ref[rows, rows] = inverse
        if k:
            step = jnp.dot(inverse, sub_ref[rows, :], precision=highest)
            before = out_ref[(k - 1) * size : k * size, : k * size]
            out_ref[rows, : k * size] = -jnp.dot(step, before, precision=highest)


def factor_inverse(diag, sub):
    total, size = diag.shape
    return pl.pallas_call(
        factor_kernel,
        out_shape=jax.ShapeDtypeStruct((total, total), f32),
        in_specs=[VMEM_SPEC] * 2,
        out_specs=VMEM_SPEC,
        scratch_shapes=[pltpu.VMEM((size, size), f32)] * (total // size),
        cost_estimate=pl.CostEstimate(flops=4 * 10**9, bytes_accessed=10**6, transcendentals=0),
        name="factor_inverse",
    )(diag, sub)


def pick_kernel(index_ref, low_ref, source_ref, out_ref):
    rows = source_ref.shape[0]
    low = low_ref[0]

    def body(i, _):
        for u in range(8):
            at = i * 8 + u
            local = index_ref[at] - low
            inside = (local >= 0) & (local < rows)
            line = source_ref[pl.ds(jnp.clip(local, 0, rows - 1), 1), :]
            out_ref[pl.ds(at, 1), :] = jnp.where(inside, line, 0.0)
        return 0

    lax.fori_loop(0, index_ref.shape[0] // 8, body, 0)


def pick(index, low, source):
    return pl.pallas_call(
        pick_kernel,
        out_shape=jax.ShapeDtypeStruct((index.shape[0], source.shape[1]), f32),
        in_specs=[SMEM_SPEC, SMEM_SPEC, VMEM_SPEC],
        out_specs=VMEM_SPEC,
        cost_estimate=pl.CostEstimate(flops=10**8, bytes_accessed=10**6, transcendentals=0),
        name="pick_rows",
    )(index, low.reshape(1), source)


def pick2_kernel(index_ref, own_ref, sib_ref, out_ref):
    half = own_ref.shape[0]

    def body(i, _):
        for u in range(8):
            at = i * 8 + u
            local = index_ref[at]
            inside = local < half
            spot = jnp.where(inside, local, local - half)
            out_ref[pl.ds(at, 1), :] = jnp.where(
                inside, own_ref[pl.ds(spot, 1), :], sib_ref[pl.ds(spot, 1), :]
            )
        return 0

    lax.fori_loop(0, index_ref.shape[0] // 8, body, 0)


def pick2(index, own, sib):
    return pl.pallas_call(
        pick2_kernel,
        out_shape=jax.ShapeDtypeStruct(own.shape, f32),
        in_specs=[SMEM_SPEC, VMEM_SPEC, VMEM_SPEC],
        out_specs=VMEM_SPEC,
        cost_estimate=pl.CostEstimate(flops=10**8, bytes_accessed=10**6, transcendentals=0),
        name="pick_merged",
    )(index, own, sib)


def interp_kernel(
    levels, index_ref, upper_ref, gram_ref, cross_ref, mine_ref, other_ref,
    leaf_out, merge_out, total_ref, *work,
):
    size = gram_ref.shape[0]
    work[0][...] = gram_ref[...]
    for j in range(levels):
        total_ref[j] = mine_ref[j] + other_ref[j]

        def body(i, _):
            for u in range(8):
                at = i * 8 + u
                work[j + 1][pl.ds(at, 1), :] = total_ref[j, pl.ds(index_ref[j, at], 1), :]
            return 0

        lax.fori_loop(0, size // 8, body, 0)
    invert_in_place(work)
    leaf_out[...] = jnp.dot(
        cross_ref[...], work[0][...], precision=highest, preferred_element_type=f32
    )
    for j in range(levels):
        rows = jnp.dot(
            total_ref[j], work[j + 1][...], precision=highest, preferred_element_type=f32
        )
        start = pl.multiple_of(upper_ref[j] * size, size)
        merge_out[j, pl.ds(start, size), :] = rows[:size]
        merge_out[j, pl.ds(pl.multiple_of(size - start, size), size), :] = rows[size:]


def interps(index, upper, gram, cross, mine, other):
    levels = index.shape[0]
    size = gram.shape[0]
    return pl.pallas_call(
        functools.partial(interp_kernel, levels),
        out_shape=(
            jax.ShapeDtypeStruct(cross.shape, f32),
            jax.ShapeDtypeStruct(mine.shape, f32),
        ),
        in_specs=[SMEM_SPEC, SMEM_SPEC] + [VMEM_SPEC] * 4,
        out_specs=(VMEM_SPEC, VMEM_SPEC),
        scratch_shapes=[pltpu.VMEM(mine.shape, f32)]
        + [pltpu.VMEM((size, size), f32)] * (levels + 1),
        cost_estimate=pl.CostEstimate(flops=4 * 10**9, bytes_accessed=10**6, transcendentals=0),
        name="interps",
    )(index, upper, gram, cross, mine, other)


def bf16_dot(left, right):
    return jnp.dot(left, right, preferred_element_type=f32)


def per_device(
    sketch,
    near_block,
    next_block,
    link_own,
    link_next,
    diag_block,
    sub_block,
    leaf_skeleton,
    merge_skeleton,
):
    rows = sketch.shape[0]
    blk_count = lax.axis_size("blk")
    blk = lax.axis_index("blk")
    leaf = lax.axis_index("leaf")
    following_half = shifted(sketch, "leaf", -1)
    previous_link = shifted(link_next, "leaf", 1)
    whole_group = gathered(sketch)
    diag_all, sub_all = gathered(diag_block), gathered(sub_block)
    links = gathered(jnp.concatenate([link_own, link_next], axis=0)[None])
    inter = link_own.shape[0]
    full_own = jnp.concatenate([links[i, :inter] for i in range(blk_count)], axis=1)
    full_next = jnp.concatenate([links[i, inter:] for i in range(blk_count)], axis=1)
    inverse = factor_inverse(diag_all, sub_all)
    near_part = bf16_dot(near_block, whole_group)
    load_part = bf16_dot(full_own, whole_group)
    following_group = gathered(following_half)
    load = load_part + bf16_dot(full_next, following_group)
    solved = jnp.dot(inverse, load, precision=highest)
    weights = lax.dot_general(inverse, solved, contract_rows, precision=highest).astype(
        jnp.bfloat16
    )
    part = inter // blk_count
    my_weights = lax.dynamic_slice_in_dim(weights, blk * part, part, 0)
    previous_half = shifted(my_weights, "leaf", 1)
    previous_weights = gathered(previous_half)
    direct = near_part + bf16_dot(next_block, following_group)
    own_back = lax.dot_general(link_own, weights, contract_rows, preferred_element_type=f32)
    from_previous = lax.dot_general(
        previous_link, previous_weights, contract_rows, preferred_element_type=f32
    )
    samples = direct - own_back - from_previous
    contrib = pick(leaf_skeleton[0], blk * rows, samples)
    chosen = contrib + from_partner(contrib, "blk", 0)
    leaf_cross = lax.dot_general(samples, chosen, contract_cols, precision=highest)
    leaf_gram = lax.dot_general(chosen, chosen, contract_cols, precision=highest)
    width = chosen.shape[1] // blk_count
    current = lax.dynamic_slice_in_dim(chosen, blk * width, width, 1)
    rank = chosen.shape[0]
    levels = merge_skeleton.shape[1]
    upper = (leaf >> jnp.arange(levels, dtype=jnp.int32)) & 1
    local_sets = (merge_skeleton[0] + rank * upper[:, None]) % (2 * rank)
    crosses = []
    for j in range(levels):
        sibling = from_partner(current, "leaf", j)
        picked = pick2(local_sets[j], current, sibling)
        crosses.append(
            lax.dot_general(
                jnp.concatenate([current, sibling], axis=0), picked, contract_cols,
                precision=highest,
            )
        )
        current = picked
    mine = jnp.stack(crosses, axis=0)
    other = from_partner(mine, "blk", 0)
    leaf_interp, merge_interp = interps(
        local_sets, upper, leaf_gram, leaf_cross, mine, other
    )
    return (samples, leaf_interp, merge_interp[None])


def solution(mesh):
    both = ("leaf", "blk")
    placed = (
        P(both, None),
        P(both, None),
        P(both, None),
        P("leaf", "blk"),
        P("leaf", "blk"),
        P(both, None),
        P(both, None),
        P("leaf", None),
        P("leaf", None, None),
    )
    return jax.shard_map(
        per_device,
        mesh=mesh,
        in_specs=placed,
        out_specs=(P(both, None), P(both, None), P(both, None, None, None)),
        check_vma=False,
    )
```

```python
import functools

import jax
import jax.numpy as jnp
from jax import lax
from jax.experimental import pallas as pl
from jax.experimental.pallas import tpu as pltpu
from jax.sharding import PartitionSpec as P

highest = lax.Precision.HIGHEST
f32 = jnp.float32
contract_rows = (((0,), (0,)), ((), ()))
contract_cols = (((1,), (1,)), ((), ()))
VMEM_SPEC = pl.BlockSpec(memory_space=pltpu.VMEM)
SMEM_SPEC = pl.BlockSpec(memory_space=pltpu.SMEM)


def shifted(block, axis, distance):
    count = lax.axis_size(axis)
    return lax.ppermute(block, axis, [((i - distance) % count, i) for i in range(count)])


def from_partner(block, axis, apart):
    count = lax.axis_size(axis)
    return lax.ppermute(block, axis, [(i, i ^ 1 << apart) for i in range(count)])


def gathered(block):
    if lax.axis_size("blk") != 2:
        return lax.all_gather(block, "blk", axis=0, tiled=True)
    other = from_partner(block, "blk", 0)
    first = lax.axis_index("blk") == 0
    return jnp.concatenate(
        [jnp.where(first, block, other), jnp.where(first, other, block)], axis=0
    )


def invert_in_place(refs, block=32):
    size = refs[0].shape[-1]
    block = min(block, size)
    lane = lax.broadcasted_iota(jnp.int32, (1, size), 1)
    row = lax.broadcasted_iota(jnp.int32, (size, 1), 0)
    inner = lax.broadcasted_iota(jnp.int32, (block, 1), 0)
    for s in range(0, size, block):
        panels = [ref[s : s + block, :] for ref in refs]
        for k in range(0, block, 2):
            at0, at1 = lane == s + k, lane == s + k + 1
            pivot_cols = at0 | at1
            for i, panel in enumerate(panels):
                col0 = jnp.broadcast_to(panel[:, s + k : s + k + 1], (block, size))
                col1 = jnp.broadcast_to(panel[:, s + k + 1 : s + k + 2], (block, size))
                r0, r1 = panel[k : k + 1, :], panel[k + 1 : k + 2, :]
                p00, p10 = col0[k : k + 1, :], col0[k + 1 : k + 2, :]
                p01, p11 = col1[k : k + 1, :], col1[k + 1 : k + 2, :]
                q0 = 1.0 / p00
                ratio = p10 * q0
                q1 = 1.0 / (p11 - ratio * p01)
                r0 = jnp.where(pivot_cols, jnp.where(at0, 1.0, 0.0), r0)
                r1 = jnp.where(pivot_cols, jnp.where(at1, 1.0, 0.0), r1)
                new1 = (r1 - ratio * r0) * q1
                new0 = (r0 - p01 * new1) * q0
                rest = jnp.where(pivot_cols, 0.0, panel) - col0 * new0 - col1 * new1
                panels[i] = jnp.where(inner == k, new0, jnp.where(inner == k + 1, new1, rest))
        outside = (lane >= s) & (lane < s + block) & ((row < s) | (row >= s + block))
        for ref, panel in zip(refs, panels):
            ref[s : s + block, :] = panel
        for ref in refs:
            value = ref[...]
            ref[...] = jnp.where(outside, 0.0, value) - jnp.dot(
                jnp.where(outside, value, 0.0), value, precision=highest
            )


def factor_kernel(diag_ref, sub_ref, out_ref, *work):
    size = diag_ref.shape[1]
    blocks = diag_ref.shape[0] // size
    row = lax.broadcasted_iota(jnp.int32, (size, size), 0)
    col = lax.broadcasted_iota(jnp.int32, (size, size), 1)
    for k in range(blocks):
        work[k][...] = jnp.where(row >= col, diag_ref[k * size : (k + 1) * size, :], 0.0)
    invert_in_place(work)
    out_ref[...] = jnp.zeros_like(out_ref)
    for k in range(blocks):
        rows = slice(k * size, (k + 1) * size)
        inverse = work[k][...]
        out_ref[rows, rows] = inverse
        if k:
            step = jnp.dot(inverse, sub_ref[rows, :], precision=highest)
            before = out_ref[(k - 1) * size : k * size, : k * size]
            out_ref[rows, : k * size] = -jnp.dot(step, before, precision=highest)


def factor_inverse(diag, sub):
    total, size = diag.shape
    return pl.pallas_call(
        factor_kernel,
        out_shape=jax.ShapeDtypeStruct((total, total), f32),
        in_specs=[VMEM_SPEC] * 2,
        out_specs=VMEM_SPEC,
        scratch_shapes=[pltpu.VMEM((size, size), f32)] * (total // size),
        cost_estimate=pl.CostEstimate(flops=4 * 10**9, bytes_accessed=10**6, transcendentals=0),
        name="factor_inverse",
    )(diag, sub)


def one_hot(column, first, count):
    spots = lax.broadcasted_iota(jnp.int32, (column.shape[0], count), 1) + first
    return jnp.where(column == spots, 1.0, 0.0)


def pick_kernel(index_ref, low_ref, source_ref, out_ref):
    chosen = one_hot(index_ref[...], low_ref[0], source_ref.shape[0])
    out_ref[...] = jnp.dot(chosen, source_ref[...], precision=highest)


def pick(index, low, source):
    return pl.pallas_call(
        pick_kernel,
        out_shape=jax.ShapeDtypeStruct((index.shape[0], source.shape[1]), f32),
        in_specs=[VMEM_SPEC, SMEM_SPEC, VMEM_SPEC],
        out_specs=VMEM_SPEC,
        cost_estimate=pl.CostEstimate(flops=10**8, bytes_accessed=10**6, transcendentals=0),
        name="pick_rows",
    )(index[:, None], low.reshape(1), source)


def pick2_kernel(index_ref, own_ref, sib_ref, out_ref):
    half = own_ref.shape[0]
    index = index_ref[...]
    out_ref[...] = jnp.dot(
        one_hot(index, 0, half), own_ref[...], precision=highest
    ) + jnp.dot(one_hot(index, half, half), sib_ref[...], precision=highest)


def pick2(index, own, sib):
    return pl.pallas_call(
        pick2_kernel,
        out_shape=jax.ShapeDtypeStruct(own.shape, f32),
        in_specs=[VMEM_SPEC] * 3,
        out_specs=VMEM_SPEC,
        cost_estimate=pl.CostEstimate(flops=10**8, bytes_accessed=10**6, transcendentals=0),
        name="pick_merged",
    )(index[:, None], own, sib)


def interp_kernel(
    levels, index_ref, upper_ref, gram_ref, cross_ref, mine_ref, other_ref,
    leaf_out, merge_out, total_ref, *work,
):
    size = gram_ref.shape[0]
    work[0][...] = gram_ref[...]
    for j in range(levels):
        total_ref[j] = mine_ref[j] + other_ref[j]

        def body(i, _):
            for u in range(8):
                at = i * 8 + u
                work[j + 1][pl.ds(at, 1), :] = total_ref[j, pl.ds(index_ref[j, at], 1), :]
            return 0

        lax.fori_loop(0, size // 8, body, 0)
    invert_in_place(work)
    leaf_out[...] = jnp.dot(
        cross_ref[...], work[0][...], precision=highest, preferred_element_type=f32
    )
    for j in range(levels):
        rows = jnp.dot(
            total_ref[j], work[j + 1][...], precision=highest, preferred_element_type=f32
        )
        start = pl.multiple_of(upper_ref[j] * size, size)
        merge_out[j, pl.ds(start, size), :] = rows[:size]
        merge_out[j, pl.ds(pl.multiple_of(size - start, size), size), :] = rows[size:]


def interps(index, upper, gram, cross, mine, other):
    levels = index.shape[0]
    size = gram.shape[0]
    return pl.pallas_call(
        functools.partial(interp_kernel, levels),
        out_shape=(
            jax.ShapeDtypeStruct(cross.shape, f32),
            jax.ShapeDtypeStruct(mine.shape, f32),
        ),
        in_specs=[SMEM_SPEC, SMEM_SPEC] + [VMEM_SPEC] * 4,
        out_specs=(VMEM_SPEC, VMEM_SPEC),
        scratch_shapes=[pltpu.VMEM(mine.shape, f32)]
        + [pltpu.VMEM((size, size), f32)] * (levels + 1),
        cost_estimate=pl.CostEstimate(flops=4 * 10**9, bytes_accessed=10**6, transcendentals=0),
        name="interps",
    )(index, upper, gram, cross, mine, other)


def bf16_dot(left, right):
    return jnp.dot(left, right, preferred_element_type=f32)


def per_device(
    sketch,
    near_block,
    next_block,
    link_own,
    link_next,
    diag_block,
    sub_block,
    leaf_skeleton,
    merge_skeleton,
):
    rows = sketch.shape[0]
    blk_count = lax.axis_size("blk")
    blk = lax.axis_index("blk")
    leaf = lax.axis_index("leaf")
    following_half = shifted(sketch, "leaf", -1)
    previous_link = shifted(link_next, "leaf", 1)
    whole_group = gathered(sketch)
    diag_all, sub_all = gathered(diag_block), gathered(sub_block)
    links = gathered(jnp.concatenate([link_own, link_next], axis=0)[None])
    inter = link_own.shape[0]
    full_own = jnp.concatenate([links[i, :inter] for i in range(blk_count)], axis=1)
    full_next = jnp.concatenate([links[i, inter:] for i in range(blk_count)], axis=1)
    inverse = factor_inverse(diag_all, sub_all)
    near_part = bf16_dot(near_block, whole_group)
    load_part = bf16_dot(full_own, whole_group)
    following_group = gathered(following_half)
    load = load_part + bf16_dot(full_next, following_group)
    solved = jnp.dot(inverse, load, precision=highest)
    weights = lax.dot_general(inverse, solved, contract_rows, precision=highest).astype(
        jnp.bfloat16
    )
    part = inter // blk_count
    my_weights = lax.dynamic_slice_in_dim(weights, blk * part, part, 0)
    previous_half = shifted(my_weights, "leaf", 1)
    previous_weights = gathered(previous_half)
    direct = near_part + bf16_dot(next_block, following_group)
    own_back = lax.dot_general(link_own, weights, contract_rows, preferred_element_type=f32)
    from_previous = lax.dot_general(
        previous_link, previous_weights, contract_rows, preferred_element_type=f32
    )
    samples = direct - own_back - from_previous
    contrib = pick(leaf_skeleton[0], blk * rows, samples)
    chosen = contrib + from_partner(contrib, "blk", 0)
    leaf_cross = lax.dot_general(samples, chosen, contract_cols, precision=highest)
    leaf_gram = lax.dot_general(chosen, chosen, contract_cols, precision=highest)
    width = chosen.shape[1] // blk_count
    current = lax.dynamic_slice_in_dim(chosen, blk * width, width, 1)
    rank = chosen.shape[0]
    levels = merge_skeleton.shape[1]
    upper = (leaf >> jnp.arange(levels, dtype=jnp.int32)) & 1
    local_sets = (merge_skeleton[0] + rank * upper[:, None]) % (2 * rank)
    crosses = []
    for j in range(levels):
        sibling = from_partner(current, "leaf", j)
        picked = pick2(local_sets[j], current, sibling)
        crosses.append(
            lax.dot_general(
                jnp.concatenate([current, sibling], axis=0), picked, contract_cols,
                precision=highest,
            )
        )
        current = picked
    mine = jnp.stack(crosses, axis=0)
    other = from_partner(mine, "blk", 0)
    leaf_interp, merge_interp = interps(
        local_sets, upper, leaf_gram, leaf_cross, mine, other
    )
    return (samples, leaf_interp, merge_interp[None])


def solution(mesh):
    both = ("leaf", "blk")
    placed = (
        P(both, None),
        P(both, None),
        P(both, None),
        P("leaf", "blk"),
        P("leaf", "blk"),
        P(both, None),
        P(both, None),
        P("leaf", None),
        P("leaf", None, None),
    )
    return jax.shard_map(
        per_device,
        mesh=mesh,
        in_specs=placed,
        out_specs=(P(both, None), P(both, None), P(both, None, None, None)),
        check_vma=False,
    )
```

```python
import functools

import jax
import jax.numpy as jnp
from jax import lax
from jax.experimental import pallas as pl
from jax.experimental.pallas import tpu as pltpu
from jax.sharding import PartitionSpec as P

highest = lax.Precision.HIGHEST
f32 = jnp.float32
contract_rows = (((0,), (0,)), ((), ()))
contract_cols = (((1,), (1,)), ((), ()))
VMEM_SPEC = pl.BlockSpec(memory_space=pltpu.VMEM)
SMEM_SPEC = pl.BlockSpec(memory_space=pltpu.SMEM)


def shifted(block, axis, distance):
    count = lax.axis_size(axis)
    return lax.ppermute(block, axis, [((i - distance) % count, i) for i in range(count)])


def from_partner(block, axis, apart):
    count = lax.axis_size(axis)
    return lax.ppermute(block, axis, [(i, i ^ 1 << apart) for i in range(count)])


def gathered(block):
    if lax.axis_size("blk") != 2:
        return lax.all_gather(block, "blk", axis=0, tiled=True)
    other = from_partner(block, "blk", 0)
    first = lax.axis_index("blk") == 0
    return jnp.concatenate(
        [jnp.where(first, block, other), jnp.where(first, other, block)], axis=0
    )


def invert_in_place(refs, block=32):
    size = refs[0].shape[-1]
    block = min(block, size)
    lane = lax.broadcasted_iota(jnp.int32, (1, size), 1)
    row = lax.broadcasted_iota(jnp.int32, (size, 1), 0)
    inner = lax.broadcasted_iota(jnp.int32, (block, 1), 0)
    for s in range(0, size, block):
        panels = [ref[s : s + block, :] for ref in refs]
        for k in range(0, block, 2):
            at0, at1 = lane == s + k, lane == s + k + 1
            pivot_cols = at0 | at1
            for i, panel in enumerate(panels):
                col0 = jnp.broadcast_to(panel[:, s + k : s + k + 1], (block, size))
                col1 = jnp.broadcast_to(panel[:, s + k + 1 : s + k + 2], (block, size))
                r0, r1 = panel[k : k + 1, :], panel[k + 1 : k + 2, :]
                p00, p10 = col0[k : k + 1, :], col0[k + 1 : k + 2, :]
                p01, p11 = col1[k : k + 1, :], col1[k + 1 : k + 2, :]
                q0 = 1.0 / p00
                ratio = p10 * q0
                q1 = 1.0 / (p11 - ratio * p01)
                r0 = jnp.where(pivot_cols, jnp.where(at0, 1.0, 0.0), r0)
                r1 = jnp.where(pivot_cols, jnp.where(at1, 1.0, 0.0), r1)
                new1 = (r1 - ratio * r0) * q1
                new0 = (r0 - p01 * new1) * q0
                rest = jnp.where(pivot_cols, 0.0, panel) - col0 * new0 - col1 * new1
                panels[i] = jnp.where(inner == k, new0, jnp.where(inner == k + 1, new1, rest))
        outside = (lane >= s) & (lane < s + block) & ((row < s) | (row >= s + block))
        for ref, panel in zip(refs, panels):
            ref[s : s + block, :] = panel
        for ref in refs:
            value = ref[...]
            ref[...] = jnp.where(outside, 0.0, value) - jnp.dot(
                jnp.where(outside, value, 0.0), value, precision=highest
            )


def factor_kernel(diag_ref, sub_ref, out_ref, *work):
    size = diag_ref.shape[1]
    blocks = diag_ref.shape[0] // size
    row = lax.broadcasted_iota(jnp.int32, (size, size), 0)
    col = lax.broadcasted_iota(jnp.int32, (size, size), 1)
    for k in range(blocks):
        work[k][...] = jnp.where(row >= col, diag_ref[k * size : (k + 1) * size, :], 0.0)
    invert_in_place(work)
    out_ref[...] = jnp.zeros_like(out_ref)
    for k in range(blocks):
        rows = slice(k * size, (k + 1) * size)
        inverse = work[k][...]
        out_ref[rows, rows] = inverse
        if k:
            step = jnp.dot(inverse, sub_ref[rows, :], precision=highest)
            before = out_ref[(k - 1) * size : k * size, : k * size]
            out_ref[rows, : k * size] = -jnp.dot(step, before, precision=highest)


def factor_inverse(diag, sub):
    total, size = diag.shape
    return pl.pallas_call(
        factor_kernel,
        out_shape=jax.ShapeDtypeStruct((total, total), f32),
        in_specs=[VMEM_SPEC] * 2,
        out_specs=VMEM_SPEC,
        scratch_shapes=[pltpu.VMEM((size, size), f32)] * (total // size),
        cost_estimate=pl.CostEstimate(flops=4 * 10**9, bytes_accessed=10**6, transcendentals=0),
        name="factor_inverse",
    )(diag, sub)


MESH = pl.DeviceIdType.MESH


def picked_rows(index, parts):
    first, total = 0, None
    for part in parts:
        count, width = part.shape
        spots = lax.broadcasted_iota(jnp.int32, (count, index.shape[1]), 0) + first
        marks = jnp.where(spots == index, 1.0, 0.0).T.astype(jnp.bfloat16)
        high = part.astype(jnp.bfloat16)
        rest = part - high.astype(f32)
        middle = rest.astype(jnp.bfloat16)
        low = (rest - middle.astype(f32)).astype(jnp.bfloat16)
        value = (
            jnp.dot(marks, high, preferred_element_type=f32)
            + jnp.dot(marks, middle, preferred_element_type=f32)
        ) + jnp.dot(marks, low, preferred_element_type=f32)
        total = value if total is None else total + value
        first = first + count
    return total


def tree_kernel(
    levels, samples_ref, leaf_set_ref, sets_ref, cross_out, gram_out, total_out,
    contrib, other, chosen, current, sibling, mine, theirs,
    swap_sem, tree_send, tree_recv, sum_send, sum_recv,
):
    leaf, blk = lax.axis_index("leaf"), lax.axis_index("blk")
    rows = samples_ref.shape[0]
    width = current.shape[2]
    mate = (leaf, 1 - blk)
    above = []
    for j in range(levels):
        bit = 1 << j
        above.append((leaf + bit - 2 * bit * ((leaf // bit) % 2), blk))
    barrier = pltpu.get_barrier_semaphore()
    for device in [mate] + above:
        pl.semaphore_signal(barrier, inc=1, device_id=device, device_id_type=MESH)

    contrib[...] = picked_rows(leaf_set_ref[...] - blk * rows, [samples_ref[...]])
    pl.semaphore_wait(barrier, levels + 1)
    swap = pltpu.make_async_remote_copy(
        src_ref=contrib, dst_ref=other, send_sem=swap_sem.at[0], recv_sem=swap_sem.at[1],
        device_id=mate, device_id_type=MESH,
    )
    swap.start()
    swap.wait()
    chosen[...] = contrib[...] + other[...]
    columns = pl.ds(pl.multiple_of(blk * width, width), width)
    current[0] = chosen[:, columns]
    sums = []

    def dots(left, right):
        return lax.dot_general(
            left, right, contract_cols, precision=highest, preferred_element_type=f32
        )

    def partial(j):
        half = current.shape[1]
        mine[j, :half, :] = dots(current[j], current[j + 1])
        mine[j, half:, :] = dots(sibling[j], current[j + 1])
        copy = pltpu.make_async_remote_copy(
            src_ref=mine.at[j], dst_ref=theirs.at[j],
            send_sem=sum_send.at[j], recv_sem=sum_recv.at[j],
            device_id=mate, device_id_type=MESH,
        )
        copy.start()
        sums.append(copy)

    def finish(j):
        sums[j].wait()
        total = mine[j] + theirs[j]
        total_out[j] = total
        gram_out[j + 1] = picked_rows(sets_ref[j : j + 1, :], [total])

    for j in range(levels):
        copy = pltpu.make_async_remote_copy(
            src_ref=current.at[j], dst_ref=sibling.at[j],
            send_sem=tree_send.at[j], recv_sem=tree_recv.at[j],
            device_id=above[j], device_id_type=MESH,
        )
        copy.start()
        if j == 0:
            gram_out[0] = dots(chosen[...], chosen[...])
            cross_out[...] = dots(samples_ref[...], chosen[...])
        else:
            partial(j - 1)
        if j > 1:
            finish(j - 2)
        copy.wait()
        current[j + 1] = picked_rows(sets_ref[j : j + 1, :], [current[j], sibling[j]])
    partial(levels - 1)
    for j in range(max(levels - 2, 0), levels):
        finish(j)


def tree(samples, leaf_set, sets):
    levels, rank = sets.shape
    rows, cols = samples.shape
    width = cols // lax.axis_size("blk")
    return pl.pallas_call(
        functools.partial(tree_kernel, levels),
        out_shape=(
            jax.ShapeDtypeStruct((rows, rank), f32),
            jax.ShapeDtypeStruct((levels + 1, rank, rank), f32),
            jax.ShapeDtypeStruct((levels, 2 * rank, rank), f32),
        ),
        in_specs=[VMEM_SPEC] * 3,
        out_specs=(VMEM_SPEC,) * 3,
        scratch_shapes=[
            pltpu.VMEM((rank, cols), f32),
            pltpu.VMEM((rank, cols), f32),
            pltpu.VMEM((rank, cols), f32),
            pltpu.VMEM((levels + 1, rank, width), f32),
            pltpu.VMEM((levels, rank, width), f32),
            pltpu.VMEM((levels, 2 * rank, rank), f32),
            pltpu.VMEM((levels, 2 * rank, rank), f32),
            pltpu.SemaphoreType.DMA((2,)),
            pltpu.SemaphoreType.DMA((levels,)),
            pltpu.SemaphoreType.DMA((levels,)),
            pltpu.SemaphoreType.DMA((levels,)),
            pltpu.SemaphoreType.DMA((levels,)),
        ],
        compiler_params=pltpu.CompilerParams(collective_id=0, has_side_effects=True),
        cost_estimate=pl.CostEstimate(flops=10**10, bytes_accessed=10**6, transcendentals=0),
        name="tree",
    )(samples, leaf_set, sets)


def interp_kernel(levels, upper_ref, gram_ref, cross_ref, total_ref, leaf_out, merge_out, *work):
    size = gram_ref.shape[1]
    for j in range(levels + 1):
        work[j][...] = gram_ref[j]
    invert_in_place(work)
    leaf_out[...] = jnp.dot(
        cross_ref[...], work[0][...], precision=highest, preferred_element_type=f32
    )
    for j in range(levels):
        rows = jnp.dot(
            total_ref[j], work[j + 1][...], precision=highest, preferred_element_type=f32
        )
        start = pl.multiple_of(upper_ref[j] * size, size)
        merge_out[j, pl.ds(start, size), :] = rows[:size]
        merge_out[j, pl.ds(pl.multiple_of(size - start, size), size), :] = rows[size:]


def interps(upper, gram, cross, total):
    levels = total.shape[0]
    size = gram.shape[1]
    return pl.pallas_call(
        functools.partial(interp_kernel, levels),
        out_shape=(
            jax.ShapeDtypeStruct(cross.shape, f32),
            jax.ShapeDtypeStruct(total.shape, f32),
        ),
        in_specs=[SMEM_SPEC] + [VMEM_SPEC] * 3,
        out_specs=(VMEM_SPEC, VMEM_SPEC),
        scratch_shapes=[pltpu.VMEM((size, size), f32)] * (levels + 1),
        cost_estimate=pl.CostEstimate(flops=4 * 10**9, bytes_accessed=10**6, transcendentals=0),
        name="interps",
    )(upper, gram, cross, total)


def bf16_dot(left, right):
    return jnp.dot(left, right, preferred_element_type=f32)


def per_device(
    sketch,
    near_block,
    next_block,
    link_own,
    link_next,
    diag_block,
    sub_block,
    leaf_skeleton,
    merge_skeleton,
):
    rows = sketch.shape[0]
    blk_count = lax.axis_size("blk")
    blk = lax.axis_index("blk")
    leaf = lax.axis_index("leaf")
    following_half = shifted(sketch, "leaf", -1)
    previous_link = shifted(link_next, "leaf", 1)
    whole_group = gathered(sketch)
    diag_all, sub_all = gathered(diag_block), gathered(sub_block)
    links = gathered(jnp.concatenate([link_own, link_next], axis=0)[None])
    inter = link_own.shape[0]
    full_own = jnp.concatenate([links[i, :inter] for i in range(blk_count)], axis=1)
    full_next = jnp.concatenate([links[i, inter:] for i in range(blk_count)], axis=1)
    inverse = factor_inverse(diag_all, sub_all)
    near_part = bf16_dot(near_block, whole_group)
    load_part = bf16_dot(full_own, whole_group)
    following_group = gathered(following_half)
    load = load_part + bf16_dot(full_next, following_group)
    solved = jnp.dot(inverse, load, precision=highest)
    weights = lax.dot_general(inverse, solved, contract_rows, precision=highest).astype(
        jnp.bfloat16
    )
    part = inter // blk_count
    my_weights = lax.dynamic_slice_in_dim(weights, blk * part, part, 0)
    previous_half = shifted(my_weights, "leaf", 1)
    previous_weights = gathered(previous_half)
    direct = near_part + bf16_dot(next_block, following_group)
    own_back = lax.dot_general(link_own, weights, contract_rows, preferred_element_type=f32)
    from_previous = lax.dot_general(
        previous_link, previous_weights, contract_rows, preferred_element_type=f32
    )
    samples = direct - own_back - from_previous
    rank = leaf_skeleton.shape[1]
    levels = merge_skeleton.shape[1]
    upper = (leaf >> jnp.arange(levels, dtype=jnp.int32)) & 1
    local_sets = (merge_skeleton[0] + rank * upper[:, None]) % (2 * rank)
    leaf_cross, grams, totals = tree(samples, leaf_skeleton, local_sets)
    leaf_interp, merge_interp = interps(upper, grams, leaf_cross, totals)
    return (samples, leaf_interp, merge_interp[None])


def solution(mesh):
    both = ("leaf", "blk")
    placed = (
        P(both, None),
        P(both, None),
        P(both, None),
        P("leaf", "blk"),
        P("leaf", "blk"),
        P(both, None),
        P(both, None),
        P("leaf", None),
        P("leaf", None, None),
    )
    return jax.shard_map(
        per_device,
        mesh=mesh,
        in_specs=placed,
        out_specs=(P(both, None), P(both, None), P(both, None, None, None)),
        check_vma=False,
    )
```
